32 devices in a mesh: seq: 32 (over z, y, x, core).
Axes of the slice: x: 2, y: 2, z: 4, core: 2. Of those that a mesh axis runs over, the one named last changes fastest.
Arguments:
- residual: bfloat16 [4096, 2560], P('seq'), may hold values from -6 to 6
- queries: bfloat16 [4096, 2560], P('seq'), may hold values from -5 to 5, as said below
- keys: bfloat16 [4096, 512], P('seq'), may hold values from -5 to 5
- values: bfloat16 [4096, 512], P('seq'), may hold values from -6 to 6
- out_proj: bfloat16 [2560, 2560], P(None, 'seq'), may hold values from -0.125 to 0.125
- norm_gain: float32 [2560], replicated, may hold values from 0.25 to 1.75
- expert_in: bfloat16 [2560, 2, 106496], P(None, None, 'seq'), may hold values from -0.125 to 0.125
- expert_down: bfloat16 [106496, 2560], P('seq'), may hold values from -0.15625 to 0.15625
- routes: int32 [4096, 2], P('seq'), may hold values from 0 to 63, all different within a row
- gate_ints: int32 [4096, 2], P('seq'), may hold values from 1 to 1023
- modality: int32 [4096], P('seq'), may hold values 0 or 1
- capacity: int32 [64, 2], replicated, may hold values from 1 to 2, as said below
Outputs:
- attended: bfloat16 [4096, 2560], P('seq')
- expert_mix: bfloat16 [4096, 2560], P('seq')
The draws below stay inside these ranges and needn't reach their ends.
Inputs may be any that keep to these rules, and one draw needn't show every extreme that they name: `queries` and `keys`: every element lies between -5 and 5. `routes`: each token names two different experts. `capacity`: some entry equals 2.
All inputs are finite; a program needn't handle non-finite values. No bound on the sum of `modality` on one device may be relied on, other than what follows from the above.
Results may differ from the reference program's by a relative error of at most 0.0086.
Values may be sent and summed in bfloat16 or wider, within the bound.
No kernel may reach another device: no remote copies, remote signals or barrier semaphores. Data moves between devices by JAX's collectives and lax.ppermute only.
A program may use at most 192 MiB of HBM per device.

```python
import math
import jax
import jax.numpy as jnp
from jax import lax

D = 2560
HEADS = 20
KV_HEADS = 4
HEAD = 128
WINDOW = 1024
EXPERTS = 64
FF = 1664
TOK_DEV = 128
CAP = 2
TOKENS = 4096
N_SEQ = 32


def draw_queries(key, part):
    drawn = jnp.clip(jax.random.normal(jax.random.fold_in(key, 3), (TOKENS, HEADS * HEAD), jnp.float32), -5.0, 5.0)
    return drawn.astype(jnp.bfloat16)


def draw_keys(key, part):
    drawn = jnp.clip(jax.random.normal(jax.random.fold_in(key, 4), (TOKENS, KV_HEADS * HEAD), jnp.float32), -5.0, 5.0)
    return drawn.astype(jnp.bfloat16)


def draw_capacity(key, part):
    cap_table = jax.random.randint(jax.random.fold_in(key, 21), (EXPERTS * 2,), 1, CAP + 1)
    full_spot = jax.random.randint(jax.random.fold_in(key, 22), (), 0, EXPERTS * 2)
    cap_table = jnp.where(jnp.arange(EXPERTS * 2) == full_spot, CAP, cap_table)
    return cap_table.reshape(EXPERTS, 2).astype(jnp.int32)


def set_ends(values, own_key, least, largest):
    longest = values.shape.index(max(values.shape))
    spots = []
    for shift in (0, 1):
        where = [jax.random.randint(jax.random.fold_in(own_key, axis), (), 0, length) for axis, length in enumerate(values.shape)]
        where[longest] = (where[longest] + shift) % values.shape[longest]
        spots.append(tuple(where))
    return values.at[spots[0]].set(least).at[spots[1]].set(largest)


def steps_of(own_key, dims, split, smallest, high):
    level = 1.0
    for axis_at, parts in split:
        heights = jax.random.uniform(jax.random.fold_in(jax.random.fold_in(own_key, 6), axis_at), (parts,), jnp.float32, smallest / len(split), high / len(split))
        level = level * jnp.repeat(jnp.exp(heights), dims[axis_at] // parts).reshape((-1,) + (1,) * (len(dims) - 1 - axis_at))
    return level


def picks_of(stream_key, rows, amount, top, lift):
    ranking = jax.random.permutation(jax.random.fold_in(stream_key, 1), amount)
    pull = ranking
    for power in range(3):
        pull = pull * pull // amount
    pull = pull * lift // amount
    lots = jax.random.randint(jax.random.fold_in(stream_key, 2), (rows, amount), 0, 4096) + pull
    fixed_rows = jax.random.permutation(jax.random.fold_in(stream_key, 3), rows)[jnp.arange(amount) % rows]
    lots = jnp.where(jnp.arange(rows)[:, None] == fixed_rows[None, :], 1 << 14, lots)
    score = lots * amount + jnp.arange(amount)
    return lax.top_k(score.astype(jnp.int32), top)[1].astype(jnp.int32)


def bell_draw(own_key, shape, deviation, bound, cuts=(), held_as=jnp.bfloat16):
    result = deviation * jax.random.normal(own_key, shape, jnp.float32)
    if cuts:
        result = result * steps_of(own_key, shape, cuts, -0.22, 0.18)
    return jnp.clip(result, -bound, bound).astype(held_as)


def setup_inputs(seed: int = 0) -> dict:
    key_list = jax.random.split(jax.random.key(seed), 13)
    return {
        "residual": bell_draw(key_list[0], (TOKENS, D), 1.0, 6.0, ((0, 32),)),
        "queries": draw_queries(jax.random.fold_in(key_list[12], 71), 0),
        "keys": draw_keys(jax.random.fold_in(key_list[12], 71), 0),
        "values": bell_draw(key_list[3], (TOKENS, KV_HEADS * HEAD), 1.0, 6.0, ((0, 32),)),
        "out_proj": bell_draw(key_list[4], (HEADS * HEAD, D), (HEADS * HEAD) ** -0.5, 0.125, ((1, 32),)),
        "norm_gain": jnp.clip(1.0 + 0.15 * jax.random.normal(key_list[5], (D,), jnp.float32), 0.25, 1.75),
        "expert_in": bell_draw(key_list[6], (D, 2, EXPERTS * FF), D ** -0.5, 0.125, ((2, 32),)),
        "expert_down": bell_draw(key_list[7], (EXPERTS * FF, D), FF ** -0.5, 0.15625, ((0, 32),)),
        "routes": picks_of(key_list[8], TOKENS, EXPERTS, 2, 512),
        "gate_ints": set_ends(jax.random.randint(key_list[9], (TOKENS, 2), 1, 1024), jax.random.fold_in(key_list[9], 1), 1, 1023).astype(jnp.int32),
        "modality": set_ends((jax.random.randint(key_list[10], (TOKENS,), 0, 2) < 1).astype(jnp.int32), jax.random.fold_in(key_list[10], 1), 0, 1),
        "capacity": draw_capacity(jax.random.fold_in(key_list[12], 71), 0),
    }


def attend(queries, keys, values):
    row_total = queries.shape[0]
    q_group = HEADS // KV_HEADS
    q_block = math.gcd(row_total, 512)
    q_blocks = queries.reshape(row_total // q_block, q_block, KV_HEADS, q_group, HEAD)
    keys_padded = jnp.pad(keys, ((WINDOW, 0), (0, 0))).reshape(row_total + WINDOW, KV_HEADS, HEAD)
    values_padded = jnp.pad(values, ((WINDOW, 0), (0, 0))).reshape(row_total + WINDOW, KV_HEADS, HEAD)

    def one_block(block_idx):
        first_row = (block_idx * q_block).astype(jnp.int32)
        q_here = lax.dynamic_index_in_dim(q_blocks, block_idx, 0, keepdims=False).astype(jnp.float32)
        k_here = lax.dynamic_slice_in_dim(keys_padded, first_row, q_block + WINDOW, 0).astype(jnp.float32)
        v_here = lax.dynamic_slice_in_dim(values_padded, first_row, q_block + WINDOW, 0).astype(jnp.float32)
        scores = jnp.einsum('qhgd,khd->hgqk', q_here, k_here) * HEAD ** (-0.5)
        q_pos = first_row + jnp.arange(q_block, dtype=jnp.int32)
        k_pos = first_row - WINDOW + jnp.arange(q_block + WINDOW, dtype=jnp.int32)
        visible = (k_pos[None, :] <= q_pos[:, None]) & (k_pos[None, :] > q_pos[:, None] - WINDOW) & (k_pos[None, :] >= 0)
        scores = jnp.where(visible, scores, -jnp.inf)
        row_max = lax.optimization_barrier(jnp.max(scores, -1, keepdims=True))
        weights_raw = jnp.exp(scores - row_max)
        probs_bf = (weights_raw / lax.optimization_barrier(jnp.sum(weights_raw, -1, keepdims=True))).astype(jnp.bfloat16)
        context = jnp.einsum('hgqk,khd->qhgd', probs_bf.astype(jnp.float32), v_here)
        return context.reshape(q_block, HEADS * HEAD).astype(jnp.bfloat16)
    mapped = lax.map(one_block, jnp.arange(row_total // q_block, dtype=jnp.int32))
    return mapped.reshape(row_total, HEADS * HEAD)

def experts_ref(normed, expert_in, expert_down, routes, gate_ints, modality, capacity):
    split_ways = max(1, N_SEQ // EXPERTS)
    slot_count = 2 * CAP
    expert = routes.reshape(N_SEQ, TOK_DEV * 2)
    mode_flag = jnp.repeat(modality, 2).reshape(N_SEQ, TOK_DEV * 2)
    slot_key = expert * 2 + mode_flag
    onehot = (slot_key[:, :, None] == jnp.arange(2 * EXPERTS, dtype=jnp.int32)[None, None, :]).astype(jnp.int32)
    before = jnp.cumsum(onehot, axis=1) - onehot
    rank_in = lax.optimization_barrier(jnp.sum(before * onehot, -1))
    limit_of = capacity.reshape(-1)[slot_key]
    kept_mask = rank_in < limit_of
    source = jnp.arange(N_SEQ, dtype=jnp.int32)[:, None]
    place_at = expert * (N_SEQ * slot_count) + source * slot_count + mode_flag * CAP + rank_in
    outside = EXPERTS * N_SEQ * slot_count
    place_at = jnp.where(kept_mask, place_at, outside).astype(jnp.int32)
    token_ids = jnp.repeat(jnp.arange(TOKENS, dtype=jnp.int32), 2)
    slot_table = jnp.full((outside,), TOKENS, jnp.int32).at[place_at.reshape(-1)].set(token_ids, mode='drop')
    slot_table = slot_table.reshape(EXPERTS, N_SEQ * slot_count)
    padded = jnp.concatenate([normed, jnp.zeros((1, D), jnp.bfloat16)], 0)
    part_width = FF // split_ways

    def one_expert(expert_id):
        picked_rows = padded[slot_table[expert_id]]
        zero_at = jnp.zeros((), jnp.int32)
        first_col = (expert_id * FF).astype(jnp.int32)
        weights_here = lax.dynamic_slice(expert_in, (zero_at, zero_at, first_col), (D, 2, FF))
        gate_val = jnp.dot(picked_rows, weights_here[:, 0, :], preferred_element_type=jnp.float32)
        up_val = jnp.dot(picked_rows, weights_here[:, 1, :], preferred_element_type=jnp.float32)
        active = (jax.nn.silu(gate_val) * up_val).astype(jnp.bfloat16)
        down_rows = lax.dynamic_slice_in_dim(expert_down, first_col, FF, 0)
        summed = jnp.zeros((N_SEQ * slot_count, D), jnp.float32)
        for piece_idx in range(split_ways):
            lo_col = piece_idx * part_width
            partial_value = jnp.dot(active[:, lo_col:lo_col + part_width], down_rows[lo_col:lo_col + part_width], preferred_element_type=jnp.float32).astype(jnp.bfloat16)
            partial_value = lax.optimization_barrier(partial_value)
            summed = summed + partial_value.astype(jnp.float32)
        return summed.astype(jnp.bfloat16)
    expert_rows = lax.map(one_expert, jnp.arange(EXPERTS, dtype=jnp.int32))
    flat_rows = expert_rows.reshape(-1, D)
    pick_at = jnp.where(kept_mask, place_at, 0).reshape(-1).astype(jnp.int32)
    chosen_rows = flat_rows[pick_at].astype(jnp.float32).reshape(TOKENS, 2, D)
    gate_scale = jnp.where(kept_mask.reshape(TOKENS, 2), gate_ints.astype(jnp.float32) / 1024.0, 0.0)
    return lax.optimization_barrier(jnp.sum(gate_scale[:, :, None] * chosen_rows, 1)).astype(jnp.bfloat16)

def reference(residual, queries, keys, values, out_proj, norm_gain, expert_in, expert_down, routes, gate_ints, modality, capacity):
    context = attend(queries, keys, values)
    attended = jnp.dot(context, out_proj, preferred_element_type=jnp.float32).astype(jnp.bfloat16)
    attended = lax.optimization_barrier(attended)
    hidden = residual.astype(jnp.float32) + attended.astype(jnp.float32)
    normed = (hidden * lax.rsqrt(lax.optimization_barrier(jnp.mean(hidden * hidden, -1, keepdims=True)) + 1e-05) * norm_gain).astype(jnp.bfloat16)
    expert_mix = experts_ref(normed, expert_in, expert_down, routes, gate_ints, modality, capacity)
    return (attended, expert_mix)
```

```python
import jax
import jax.numpy as jnp
from jax import lax
from jax.experimental import pallas as pl
from jax.experimental.pallas import tpu as pltpu
from jax.sharding import PartitionSpec as P

HEADS = 20
KV_HEADS = 4
HEAD = 128
WINDOW = 1024
EXPERTS = 64
CAP = 2
SLOTS = 2 * CAP
VMEM_LIMIT = 60 * 1024 * 1024
F32 = jnp.float32
BF16 = jnp.bfloat16
NT = (((1,), (1,)), ((), ()))


def swap(value, mask):
    count = lax.axis_size("seq")
    return lax.ppermute(value, "seq", [(i, i ^ mask) for i in range(count)])


def shift(value, steps):
    count = lax.axis_size("seq")
    return lax.ppermute(value, "seq", [(i, i + steps) for i in range(count - steps)])


def window_blocks(kv, pos, back):
    count = lax.axis_size("seq")
    if back != 8 or count % back:
        found = [(shift(kv, s), pos - s) for s in range(back, 0, -1) if s < count]
        return found + [(kv, pos)]
    group = pos // back
    chip = (pos % back) // 2
    core = pos % 2
    prev = shift(kv, back) if count > back else jnp.zeros_like(kv)
    blocks = [(kv, pos), (prev, pos - back)]
    mate = swap(jnp.where(core == 1, prev, kv), 1)
    blocks.append((mate, jnp.where(core == 0, pos + 1 - back, pos - 1)))
    for m in range(1, back // 2):
        other = chip ^ m
        got = swap(jnp.where(chip < other, kv, prev), 2 * m)
        base = jnp.where(other < chip, group, group - 1) * back + 2 * other
        blocks.append((got, base + core))
        blocks.append((swap(got, 1), base + 1 - core))
    return blocks


def attention_body(count, off_ref, q_ref, *refs):
    k_refs, v_refs, o_ref = refs[:count], refs[count : 2 * count], refs[2 * count]
    rows = q_ref.shape[0]
    group = q_ref.shape[1] // HEAD
    delta = lax.broadcasted_iota(jnp.int32, (rows, rows), 0) - lax.broadcasted_iota(
        jnp.int32, (rows, rows), 1
    )
    bias = []
    for b in range(count):
        d = delta + off_ref[b] * rows
        bias.append(jnp.where((d >= 0) & (d < WINDOW), 0.0, -jnp.inf))
    bias = jnp.concatenate(bias, 1)
    k_all = jnp.concatenate([r[...] for r in k_refs], 0)
    v_all = jnp.concatenate([r[...] for r in v_refs], 0)
    scale = HEAD ** (-0.5) * 1.4426950408889634
    for g in range(group):
        cols = slice(g * HEAD, (g + 1) * HEAD)
        s = lax.dot_general(q_ref[:, cols], k_all, NT, preferred_element_type=F32) + bias
        top = jnp.max(s, -1, keepdims=True)
        w = jnp.exp2((s - top) * scale)
        total = jnp.sum(w, -1, keepdims=True)
        out = jnp.dot(w.astype(BF16), v_all, preferred_element_type=F32)
        o_ref[:, cols] = (out * (1.0 / total)).astype(BF16)


def attention(queries, blocks, offsets):
    rows = queries.shape[0]
    count = len(blocks)
    wide = HEADS // KV_HEADS * HEAD
    k_spec = pl.BlockSpec((rows, HEAD), lambda h: (0, h))
    v_spec = pl.BlockSpec((rows, HEAD), lambda h: (0, h + KV_HEADS))

    def body(*refs):
        attention_body(count, *refs)

    return pl.pallas_call(
        body,
        grid=(KV_HEADS,),
        in_specs=[
            pl.BlockSpec(memory_space=pltpu.SMEM),
            pl.BlockSpec((rows, wide), lambda h: (0, h)),
        ]
        + [k_spec] * count
        + [v_spec] * count,
        out_specs=pl.BlockSpec((rows, wide), lambda h: (0, h)),
        out_shape=jax.ShapeDtypeStruct(queries.shape, BF16),
        compiler_params=pltpu.CompilerParams(vmem_limit_bytes=VMEM_LIMIT),
        name="attention",
    )(offsets, queries, *blocks, *blocks)


def project_body(ctx_ref, w_ref, res_ref, gain_ref, sel_ref, att_ref, slot_ref, hid_ref, sq_ref):
    step = pl.program_id(0)
    att = lax.dot_general(ctx_ref[...], w_ref[...], NT, preferred_element_type=F32).astype(BF16)
    att_ref[...] = att
    hid = res_ref[...].astype(F32) + att.astype(F32)
    hid_ref[step] = hid
    part = jnp.sum(hid * hid, -1, keepdims=True)

    @pl.when(step == 0)
    def _():
        sq_ref[...] = part

    @pl.when(step > 0)
    def _():
        sq_ref[...] += part

    @pl.when(step == pl.num_programs(0) - 1)
    def _():
        width = hid_ref.shape[2]
        total = hid_ref.shape[0] * width
        inv = lax.rsqrt(sq_ref[...] / total + 1e-05)
        for c in range(hid_ref.shape[0]):
            cols = slice(c * width, (c + 1) * width)
            normed = (hid_ref[c] * inv * gain_ref[:, cols]).astype(BF16)
            slot_ref[:, cols] = jnp.dot(
                sel_ref[...], normed, preferred_element_type=F32
            ).astype(BF16)


def project(context, weight_t, residual, gain, select):
    rows, width = residual.shape
    nb = 512
    steps = width // nb
    return pl.pallas_call(
        project_body,
        grid=(steps,),
        in_specs=[
            pl.BlockSpec(context.shape, lambda j: (0, 0)),
            pl.BlockSpec((nb, context.shape[1]), lambda j: (j, 0)),
            pl.BlockSpec((rows, nb), lambda j: (0, j)),
            pl.BlockSpec((1, width), lambda j: (0, 0)),
            pl.BlockSpec(select.shape, lambda j: (0, 0)),
        ],
        out_specs=[
            pl.BlockSpec((rows, nb), lambda j: (0, j)),
            pl.BlockSpec((select.shape[0], width), lambda j: (0, 0)),
        ],
        out_shape=[
            jax.ShapeDtypeStruct((rows, width), BF16),
            jax.ShapeDtypeStruct((select.shape[0], width), BF16),
        ],
        scratch_shapes=[pltpu.VMEM((steps, rows, nb), F32), pltpu.VMEM((rows, 1), F32)],
        compiler_params=pltpu.CompilerParams(vmem_limit_bytes=VMEM_LIMIT),
        name="project",
    )(context, weight_t, residual, gain, select)


def experts_body(local, x_ref, up_hbm, down_hbm, o_ref, up_ref, down_ref, wide_ref, acc_ref, up_sem, down_sem):
    total, width = x_ref.shape
    rows = total // local
    hidden = up_ref.shape[3]
    chunks = up_sem.shape[1]
    depth = width // chunks
    parts = down_sem.shape[1]
    tall = hidden // parts

    def up_copy(e, k):
        return pltpu.make_async_copy(
            up_hbm.at[pl.ds(k * depth, depth), :, pl.ds(e * hidden, hidden)],
            up_ref.at[e, pl.ds(k * depth, depth)],
            up_sem.at[e, k],
        )

    def down_copy(e, k):
        return pltpu.make_async_copy(
            down_hbm.at[pl.ds(e * hidden + k * tall, tall)],
            down_ref.at[e, pl.ds(k * tall, tall)],
            down_sem.at[e, k],
        )

    for e in range(local):
        for k in range(chunks):
            up_copy(e, k).start()
        for k in range(parts):
            down_copy(e, k).start()

    row = lax.broadcasted_iota(jnp.int32, (rows, total), 0)
    col = lax.broadcasted_iota(jnp.int32, (rows, total), 1)
    lane = lax.broadcasted_iota(jnp.int32, (HEAD, 2 * HEAD), 1)
    sub = lax.broadcasted_iota(jnp.int32, (HEAD, 2 * HEAD), 0)
    spread = [jnp.where(lane == 2 * sub + j, 1.0, 0.0).astype(BF16) for j in range(2)]
    per = SLOTS * local
    picks = [
        jnp.where(col == (row // SLOTS) * per + e * SLOTS + row % SLOTS, 1.0, 0.0).astype(BF16)
        for e in range(local)
    ]
    for e in range(local):
        for k in range(chunks):
            mine = jnp.dot(
                picks[e], x_ref[:, k * depth : (k + 1) * depth], preferred_element_type=F32
            ).astype(BF16)
            for c in range(depth // HEAD):
                piece = mine[:, c * HEAD : (c + 1) * HEAD]
                for j in range(2):
                    wide_ref[k, j * rows : (j + 1) * rows, 2 * c * HEAD : 2 * (c + 1) * HEAD] = jnp.dot(
                        piece, spread[j], preferred_element_type=F32
                    ).astype(BF16)

        def up_step(k, carry):
            up_copy(e, k).wait()
            w = up_ref[e, pl.ds(k * depth, depth)].reshape(2 * depth, hidden)
            prod = jnp.dot(wide_ref[k], w, preferred_element_type=F32)

            @pl.when(k == 0)
            def _():
                acc_ref[...] = prod

            @pl.when(k > 0)
            def _():
                acc_ref[...] += prod

            return carry

        lax.fori_loop(0, chunks, up_step, 0)
        gate = acc_ref[:rows]
        act = (gate * jax.nn.sigmoid(gate) * acc_ref[rows:]).astype(BF16)
        for k in range(parts):
            down_copy(e, k).wait()
        out = jnp.dot(act, down_ref[e], preferred_element_type=F32).astype(BF16)
        back = lax.dot_general(
            picks[e], out, (((0,), (0,)), ((), ())), preferred_element_type=F32
        ).astype(BF16)
        if e == 0:
            o_ref[...] = back
        else:
            o_ref[...] = o_ref[...] + back


def experts(x, up, down, local):
    total, width = x.shape
    hidden = up.shape[2] // local
    chunks = 10
    parts = 4
    any_spec = pl.BlockSpec(memory_space=pl.ANY)

    def body(*refs):
        experts_body(local, *refs)

    return pl.pallas_call(
        body,
        in_specs=[pl.BlockSpec(memory_space=pltpu.VMEM), any_spec, any_spec],
        out_specs=pl.BlockSpec(memory_space=pltpu.VMEM),
        out_shape=jax.ShapeDtypeStruct((total, width), BF16),
        scratch_shapes=[
            pltpu.VMEM((local, width, 2, hidden), BF16),
            pltpu.VMEM((local, hidden, width), BF16),
            pltpu.VMEM((chunks, 2 * total // local, 2 * width // chunks), BF16),
            pltpu.VMEM((2 * total // local, hidden), F32),
            pltpu.SemaphoreType.DMA((local, chunks)),
            pltpu.SemaphoreType.DMA((local, parts)),
        ],
        compiler_params=pltpu.CompilerParams(vmem_limit_bytes=VMEM_LIMIT),
        name="experts",
    )(x, up, down)


def experts_plain(x, up, down, local):
    total, width = x.shape
    hidden = up.shape[2] // local
    rows = x.reshape(-1, local, SLOTS, width)
    pair = jnp.einsum(
        "nlkd,dglf->glnkf",
        rows,
        up.reshape(width, 2, local, hidden),
        preferred_element_type=F32,
    )
    act = (jax.nn.silu(pair[0]) * pair[1]).astype(BF16)
    part = jnp.einsum(
        "lnkf,lfd->nlkd", act, down.reshape(local, hidden, width), preferred_element_type=F32
    )
    return part.astype(BF16).reshape(total, width)


def combine_body(high_ref, low_ref, r_ref, o_ref):
    r = r_ref[...]
    o_ref[...] = (
        jnp.dot(high_ref[...], r, preferred_element_type=F32)
        + jnp.dot(low_ref[...], r, preferred_element_type=F32)
    ).astype(BF16)


def combine(high, low, rows):
    width = rows.shape[1]
    nb = 1280
    same = lambda j: (0, 0)
    return pl.pallas_call(
        combine_body,
        grid=(width // nb,),
        in_specs=[
            pl.BlockSpec(high.shape, same),
            pl.BlockSpec(low.shape, same),
            pl.BlockSpec((rows.shape[0], nb), lambda j: (0, j)),
        ],
        out_specs=pl.BlockSpec((high.shape[0], nb), lambda j: (0, j)),
        out_shape=jax.ShapeDtypeStruct((high.shape[0], width), BF16),
        compiler_params=pltpu.CompilerParams(vmem_limit_bytes=VMEM_LIMIT),
        name="combine",
    )(high, low, rows)


def routing(routes, gate_ints, modality, capacity):
    tokens = routes.shape[0]
    key = (routes * 2 + modality[:, None]).reshape(-1)
    order = jnp.arange(2 * tokens, dtype=jnp.int32)
    same = (key[:, None] == key[None, :]) & (order[None, :] < order[:, None])
    rank = jnp.sum(same.astype(jnp.int32), 1)
    hot = key[:, None] == jnp.arange(2 * EXPERTS, dtype=jnp.int32)[None, :]
    limit = jnp.sum(jnp.where(hot, capacity.reshape(1, -1), 0), 1)
    spot = jnp.where(rank < limit, key * CAP + rank, -1).reshape(tokens, 2)
    slot = jnp.arange(EXPERTS * SLOTS, dtype=jnp.int32)
    select = (spot[None, :, 0] == slot[:, None]) | (spot[None, :, 1] == slot[:, None])
    place = spot[:, :, None] == slot[None, None, :]
    low = gate_ints % 8
    high = jnp.sum(jnp.where(place, (gate_ints - low)[:, :, None], 0), 1)
    low = jnp.sum(jnp.where(place, low[:, :, None], 0), 1)
    to_gate = lambda v: (v.astype(F32) / 1024.0).astype(BF16)
    return select.astype(BF16), to_gate(high), to_gate(low)


def body(
    residual,
    queries,
    keys,
    values,
    out_proj,
    norm_gain,
    expert_in,
    expert_down,
    routes,
    gate_ints,
    modality,
    capacity,
):
    devices = lax.axis_size("seq")
    pos = lax.axis_index("seq")
    rows, width = residual.shape
    back = (WINDOW + rows - 1) // rows
    blocks = window_blocks(jnp.concatenate([keys, values], 1), pos, back)
    offsets = jnp.stack([jnp.where(b < 0, 4 * back, pos - b) for _, b in blocks]).astype(jnp.int32)
    weight_t = lax.all_gather(out_proj.T, "seq", axis=0, tiled=True)
    select, high, low = routing(routes, gate_ints, modality, capacity)
    context = attention(queries, [v for v, _ in blocks], offsets)
    attended, slots = project(context, weight_t, residual, norm_gain.reshape(1, width), select)
    ways = max(1, devices // EXPERTS)
    local = max(1, EXPERTS // devices)
    if ways > 1:
        slots = jnp.repeat(slots.reshape(EXPERTS, SLOTS, width), ways, 0)
    outgoing = slots.reshape(devices, local * SLOTS, width)
    arrived = lax.all_to_all(outgoing, "seq", split_axis=0, concat_axis=0, tiled=True)
    arrived = arrived.reshape(devices * local * SLOTS, width)
    if expert_in.shape[2] % (local * HEAD) == 0:
        computed = experts(arrived, expert_in, expert_down, local)
    else:
        computed = experts_plain(arrived, expert_in, expert_down, local)
    computed = lax.optimization_barrier(computed)
    returned = lax.all_to_all(
        computed.reshape(devices, local * SLOTS, width), "seq", split_axis=0, concat_axis=0, tiled=True
    )
    if ways > 1:
        parts = returned.reshape(EXPERTS, ways, SLOTS, width).astype(F32)
        returned = jnp.sum(parts, 1).astype(BF16)
    expert_mix = combine(high, low, returned.reshape(EXPERTS * SLOTS, width))
    return (attended, expert_mix)


def solution(mesh):
    placed = (
        P("seq", None),
        P("seq", None),
        P("seq", None),
        P("seq", None),
        P(None, "seq"),
        P(),
        P(None, None, "seq"),
        P("seq", None),
        P("seq", None),
        P("seq", None),
        P("seq"),
        P(),
    )
    return jax.shard_map(
        body,
        mesh=mesh,
        in_specs=placed,
        out_specs=(P("seq", None), P("seq", None)),
        check_vma=False,
    )
```

```python
import jax
import jax.numpy as jnp
from jax import lax
from jax.experimental import pallas as pl
from jax.experimental.pallas import tpu as pltpu
from jax.sharding import PartitionSpec as P


HEADS = 20
KV_HEADS = 4
HEAD = 128
WINDOW = 1024
EXPERTS = 64
CAP = 2
SLOTS = 2 * CAP
VMEM_LIMIT = 60 * 1024 * 1024
F32 = jnp.float32
BF16 = jnp.bfloat16
NT = (((1,), (1,)), ((), ()))


def swap(value, mask):
    count = lax.axis_size("seq")
    return lax.ppermute(value, "seq", [(i, i ^ mask) for i in range(count)])


def shift(value, steps):
    count = lax.axis_size("seq")
    return lax.ppermute(value, "seq", [(i, i + steps) for i in range(count - steps)])


def window_blocks(kv, pos, back):
    count = lax.axis_size("seq")
    if back != 8 or count % back:
        found = [(shift(kv, s), pos - s) for s in range(back, 0, -1) if s < count]
        return found + [(kv, pos)]
    group = pos // back
    chip = (pos % back) // 2
    core = pos % 2
    prev = shift(kv, back) if count > back else jnp.zeros_like(kv)
    blocks = [(kv, pos), (prev, pos - back)]
    mate = swap(jnp.where(core == 1, prev, kv), 1)
    blocks.append((mate, jnp.where(core == 0, pos + 1 - back, pos - 1)))
    for m in range(1, back // 2):
        other = chip ^ m
        got = swap(jnp.where(chip < other, kv, prev), 2 * m)
        base = jnp.where(other < chip, group, group - 1) * back + 2 * other
        blocks.append((got, base + core))
        blocks.append((swap(got, 1), base + 1 - core))
    return blocks


def attention_body(count, off_ref, q_ref, *refs):
    k_refs, v_refs, o_ref = refs[:count], refs[count : 2 * count], refs[2 * count]
    rows = q_ref.shape[0]
    group = q_ref.shape[1] // HEAD
    delta = lax.broadcasted_iota(jnp.int32, (rows, rows), 0) - lax.broadcasted_iota(
        jnp.int32, (rows, rows), 1
    )
    bias = []
    for b in range(count):
        d = delta + off_ref[b] * rows
        bias.append(jnp.where((d >= 0) & (d < WINDOW), 0.0, -jnp.inf))
    bias = jnp.concatenate(bias, 1)
    k_all = jnp.concatenate([r[...] for r in k_refs], 0)
    v_all = jnp.concatenate([r[...] for r in v_refs], 0)
    scale = HEAD ** (-0.5) * 1.4426950408889634
    for g in range(group):
        cols = slice(g * HEAD, (g + 1) * HEAD)
        s = lax.dot_general(q_ref[:, cols], k_all, NT, preferred_element_type=F32) + bias
        top = jnp.max(s, -1, keepdims=True)
        w = jnp.exp2((s - top) * scale)
        total = jnp.sum(w, -1, keepdims=True)
        out = jnp.dot(w.astype(BF16), v_all, preferred_element_type=F32)
        o_ref[:, cols] = (out * (1.0 / total)).astype(BF16)


def attention(queries, blocks, offsets):
    rows = queries.shape[0]
    count = len(blocks)
    wide = HEADS // KV_HEADS * HEAD
    k_spec = pl.BlockSpec((rows, HEAD), lambda h: (0, h))
    v_spec = pl.BlockSpec((rows, HEAD), lambda h: (0, h + KV_HEADS))

    def body(*refs):
        attention_body(count, *refs)

    return pl.pallas_call(
        body,
        grid=(KV_HEADS,),
        in_specs=[
            pl.BlockSpec(memory_space=pltpu.SMEM),
            pl.BlockSpec((rows, wide), lambda h: (0, h)),
        ]
        + [k_spec] * count
        + [v_spec] * count,
        out_specs=pl.BlockSpec((rows, wide), lambda h: (0, h)),
        out_shape=jax.ShapeDtypeStruct(queries.shape, BF16),
        compiler_params=pltpu.CompilerParams(vmem_limit_bytes=VMEM_LIMIT),
        name="attention",
    )(offsets, queries, *blocks, *blocks)


def project_body(ctx_ref, w_ref, res_ref, gain_ref, sel_ref, att_ref, slot_ref, hid_ref, sq_ref):
    step = pl.program_id(0)
    att = lax.dot_general(ctx_ref[...], w_ref[...], NT, preferred_element_type=F32).astype(BF16)
    att_ref[...] = att
    hid = res_ref[...].astype(F32) + att.astype(F32)
    hid_ref[step] = hid
    part = jnp.sum(hid * hid, -1, keepdims=True)

    @pl.when(step == 0)
    def _():
        sq_ref[...] = part

    @pl.when(step > 0)
    def _():
        sq_ref[...] += part

    @pl.when(step == pl.num_programs(0) - 1)
    def _():
        width = hid_ref.shape[2]
        total = hid_ref.shape[0] * width
        inv = lax.rsqrt(sq_ref[...] / total + 1e-05)
        for c in range(hid_ref.shape[0]):
            cols = slice(c * width, (c + 1) * width)
            normed = (hid_ref[c] * inv * gain_ref[:, cols]).astype(BF16)
            slot_ref[:, cols] = jnp.dot(
                sel_ref[...], normed, preferred_element_type=F32
            ).astype(BF16)


def project(context, weight_t, residual, gain, select):
    rows, width = residual.shape
    nb = 512
    steps = width // nb
    return pl.pallas_call(
        project_body,
        grid=(steps,),
        in_specs=[
            pl.BlockSpec(context.shape, lambda j: (0, 0)),
            pl.BlockSpec((nb, context.shape[1]), lambda j: (j, 0)),
            pl.BlockSpec((rows, nb), lambda j: (0, j)),
            pl.BlockSpec((1, width), lambda j: (0, 0)),
            pl.BlockSpec(select.shape, lambda j: (0, 0)),
        ],
        out_specs=[
            pl.BlockSpec((rows, nb), lambda j: (0, j)),
            pl.BlockSpec((select.shape[0], width), lambda j: (0, 0)),
        ],
        out_shape=[
            jax.ShapeDtypeStruct((rows, width), BF16),
            jax.ShapeDtypeStruct((select.shape[0], width), BF16),
        ],
        scratch_shapes=[pltpu.VMEM((steps, rows, nb), F32), pltpu.VMEM((rows, 1), F32)],
        compiler_params=pltpu.CompilerParams(vmem_limit_bytes=VMEM_LIMIT),
        name="project",
    )(context, weight_t, residual, gain, select)


def gather_weight(own, back):
    count = lax.axis_size("seq")
    groups = count // back
    rows = own.shape[0]
    cut = rows // 32 * 16 + 16
    turn = [(i, (i + back) % count) for i in range(count)]

    def onward(value):
        return lax.ppermute(value, "seq", turn)

    x, y = swap(own, 2), swap(own, 4)
    far = jnp.concatenate([swap(y[:cut], 2), swap(x[cut:], 4)], 0)
    found = [[own, x, y, far]]
    for _ in range(1, groups):
        own = onward(own)
        far = onward(far)
        found.append([own, swap(own, 2), swap(own, 4), far])
    return found


def half_body(groups, where_ref, mine_ref, other_ref, *refs):
    bufs = refs[: 4 * groups]
    keep_ref, send_ref, w_ref, sem = refs[4 * groups :]
    tall = w_ref.shape[1]
    group, chip = where_ref[0], where_ref[1]
    rows = bufs[0].shape[0]
    used = 4 * rows

    def copies(s):
        slot = lax.rem(group - s + groups, groups)
        for m in range(4):
            to = pl.multiple_of((chip ^ m) * rows, 16)
            yield pltpu.make_async_copy(
                bufs[4 * s + m], w_ref.at[slot, pl.ds(to, rows)], sem.at[s, m]
            )

    for s in range(groups):
        for c in copies(s):
            c.start()
    for s in range(groups):
        w_ref[s, used:] = jnp.zeros((tall - used, w_ref.shape[2]), BF16)
    both = jnp.concatenate([mine_ref[...], other_ref[...]], 0)
    half = mine_ref.shape[0]
    for s in range(groups):
        for c in copies(s):
            c.wait()
        slot = lax.rem(group - s + groups, groups)
        out = lax.dot_general(both, w_ref[slot], NT, preferred_element_type=F32).astype(BF16)
        keep_ref[slot] = out[:half]
        send_ref[slot] = out[half:]


def project_half(where, mine, other, found):
    groups = len(found)
    bufs = [b for row in found for b in row]
    tall = -(-4 * bufs[0].shape[0] // HEAD) * HEAD
    tokens, width = mine.shape
    shape = jax.ShapeDtypeStruct((groups, tokens, tall), BF16)

    def body(*refs):
        half_body(groups, *refs)

    vmem = pl.BlockSpec(memory_space=pltpu.VMEM)
    return pl.pallas_call(
        body,
        in_specs=[pl.BlockSpec(memory_space=pltpu.SMEM), vmem, vmem]
        + [pl.BlockSpec(memory_space=pltpu.HBM)] * len(bufs),
        out_specs=[vmem, vmem],
        out_shape=[shape, shape],
        scratch_shapes=[
            pltpu.VMEM((groups, tall, width), BF16),
            pltpu.SemaphoreType.DMA((groups, 4)),
        ],
        compiler_params=pltpu.CompilerParams(vmem_limit_bytes=VMEM_LIMIT),
        name="project_half",
    )(where, mine, other, *bufs)


def merge_body(rows, where_ref, mine_ref, their_ref, res_ref, gain_ref, sel_ref, att_ref, slot_ref, hid_ref):
    groups, tokens, tall = mine_ref.shape
    wide = 8 * rows
    core = where_ref[2]
    line = lax.broadcasted_iota(jnp.int32, (tall, wide), 0)
    col = lax.broadcasted_iota(jnp.int32, (tall, wide), 1)
    pair, rest = col // (2 * rows), col % (2 * rows)
    side = jnp.where(rest >= rows, 1, 0)
    hit = line == pair * rows + rest - side * rows
    pick_mine = jnp.where(hit & (side == core), 1.0, 0.0).astype(BF16)
    pick_their = jnp.where(hit & (side != core), 1.0, 0.0).astype(BF16)
    square = jnp.zeros((tokens, 1), F32)
    for g in range(groups):
        cols = slice(g * wide, (g + 1) * wide)
        att = jnp.dot(mine_ref[g], pick_mine, preferred_element_type=F32) + jnp.dot(
            their_ref[g], pick_their, preferred_element_type=F32
        )
        att_ref[:, cols] = att.astype(BF16)
        hid = res_ref[:, cols].astype(F32) + att
        hid_ref[:, cols] = hid
        square += jnp.sum(hid * hid, -1, keepdims=True)
    inv = lax.rsqrt(square / (groups * wide) + 1e-05)
    for g in range(groups):
        cols = slice(g * wide, (g + 1) * wide)
        normed = (hid_ref[:, cols] * inv * gain_ref[:, cols]).astype(BF16)
        slot_ref[:, cols] = jnp.dot(sel_ref[...], normed, preferred_element_type=F32).astype(BF16)


def merge(where, mine, theirs, residual, gain, select, rows):
    tokens, width = residual.shape
    vmem = pl.BlockSpec(memory_space=pltpu.VMEM)

    def body(*refs):
        merge_body(rows, *refs)

    return pl.pallas_call(
        body,
        in_specs=[pl.BlockSpec(memory_space=pltpu.SMEM)] + [vmem] * 5,
        out_specs=[vmem, vmem],
        out_shape=[
            jax.ShapeDtypeStruct((tokens, width), BF16),
            jax.ShapeDtypeStruct((select.shape[0], width), BF16),
        ],
        scratch_shapes=[pltpu.VMEM((tokens, width), F32)],
        compiler_params=pltpu.CompilerParams(vmem_limit_bytes=VMEM_LIMIT),
        name="merge",
    )(where, mine, theirs, residual, gain, select)


def experts_body(local, x_ref, up_hbm, down_hbm, o_ref, up_ref, down_ref, wide_ref, acc_ref, up_sem, down_sem):
    total, width = x_ref.shape
    rows = total // local
    hidden = up_ref.shape[3]
    chunks = up_sem.shape[1]
    depth = width // chunks
    parts = down_sem.shape[1]
    tall = hidden // parts

    def up_copy(e, k):
        return pltpu.make_async_copy(
            up_hbm.at[pl.ds(k * depth, depth), :, pl.ds(e * hidden, hidden)],
            up_ref.at[e, pl.ds(k * depth, depth)],
            up_sem.at[e, k],
        )

    def down_copy(e, k):
        return pltpu.make_async_copy(
            down_hbm.at[pl.ds(e * hidden + k * tall, tall)],
            down_ref.at[e, pl.ds(k * tall, tall)],
            down_sem.at[e, k],
        )

    for e in range(local):
        for k in range(chunks):
            up_copy(e, k).start()
        for k in range(parts):
            down_copy(e, k).start()

    row = lax.broadcasted_iota(jnp.int32, (rows, total), 0)
    col = lax.broadcasted_iota(jnp.int32, (rows, total), 1)
    lane = lax.broadcasted_iota(jnp.int32, (HEAD, 2 * HEAD), 1)
    sub = lax.broadcasted_iota(jnp.int32, (HEAD, 2 * HEAD), 0)
    spread = [jnp.where(lane == 2 * sub + j, 1.0, 0.0).astype(BF16) for j in range(2)]
    per = SLOTS * local
    picks = [
        jnp.where(col == (row // SLOTS) * per + e * SLOTS + row % SLOTS, 1.0, 0.0).astype(BF16)
        for e in range(local)
    ]
    for e in range(local):
        for k in range(chunks):
            mine = jnp.dot(
                picks[e], x_ref[:, k * depth : (k + 1) * depth], preferred_element_type=F32
            ).astype(BF16)
            for c in range(depth // HEAD):
                piece = mine[:, c * HEAD : (c + 1) * HEAD]
                for j in range(2):
                    wide_ref[k, j * rows : (j + 1) * rows, 2 * c * HEAD : 2 * (c + 1) * HEAD] = jnp.dot(
                        piece, spread[j], preferred_element_type=F32
                    ).astype(BF16)

        for k in range(chunks):
            up_copy(e, k).wait()
            w = up_ref[e, pl.ds(k * depth, depth)].reshape(2 * depth, hidden)
            prod = jnp.dot(wide_ref[k], w, preferred_element_type=F32)
            if k == 0:
                acc_ref[...] = prod
            else:
                acc_ref[...] += prod
        gate = acc_ref[:rows]
        act = (gate * jax.nn.sigmoid(gate) * acc_ref[rows:]).astype(BF16)
        for k in range(parts):
            down_copy(e, k).wait()
        out = jnp.dot(act, down_ref[e], preferred_element_type=F32).astype(BF16)
        back = lax.dot_general(
            picks[e], out, (((0,), (0,)), ((), ())), preferred_element_type=F32
        ).astype(BF16)
        if e == 0:
            o_ref[...] = back
        else:
            o_ref[...] = o_ref[...] + back


def experts(x, up, down, local):
    total, width = x.shape
    hidden = up.shape[2] // local
    chunks = 5
    parts = 4
    any_spec = pl.BlockSpec(memory_space=pl.ANY)

    def body(*refs):
        experts_body(local, *refs)

    return pl.pallas_call(
        body,
        in_specs=[pl.BlockSpec(memory_space=pltpu.VMEM), any_spec, any_spec],
        out_specs=pl.BlockSpec(memory_space=pltpu.VMEM),
        out_shape=jax.ShapeDtypeStruct((total, width), BF16),
        scratch_shapes=[
            pltpu.VMEM((local, width, 2, hidden), BF16),
            pltpu.VMEM((local, hidden, width), BF16),
            pltpu.VMEM((chunks, 2 * total // local, 2 * width // chunks), BF16),
            pltpu.VMEM((2 * total // local, hidden), F32),
            pltpu.SemaphoreType.DMA((local, chunks)),
            pltpu.SemaphoreType.DMA((local, parts)),
        ],
        compiler_params=pltpu.CompilerParams(vmem_limit_bytes=VMEM_LIMIT),
        name="experts",
    )(x, up, down)


def experts_plain(x, up, down, local):
    total, width = x.shape
    hidden = up.shape[2] // local
    rows = x.reshape(-1, local, SLOTS, width)
    pair = jnp.einsum(
        "nlkd,dglf->glnkf",
        rows,
        up.reshape(width, 2, local, hidden),
        preferred_element_type=F32,
    )
    act = (jax.nn.silu(pair[0]) * pair[1]).astype(BF16)
    part = jnp.einsum(
        "lnkf,lfd->nlkd", act, down.reshape(local, hidden, width), preferred_element_type=F32
    )
    return part.astype(BF16).reshape(total, width)


def combine_body(high_ref, low_ref, r_ref, o_ref):
    r = r_ref[...]
    o_ref[...] = (
        jnp.dot(high_ref[...], r, preferred_element_type=F32)
        + jnp.dot(low_ref[...], r, preferred_element_type=F32)
    ).astype(BF16)


def combine(high, low, rows):
    width = rows.shape[1]
    nb = 1280
    same = lambda j: (0, 0)
    return pl.pallas_call(
        combine_body,
        grid=(width // nb,),
        in_specs=[
            pl.BlockSpec(high.shape, same),
            pl.BlockSpec(low.shape, same),
            pl.BlockSpec((rows.shape[0], nb), lambda j: (0, j)),
        ],
        out_specs=pl.BlockSpec((high.shape[0], nb), lambda j: (0, j)),
        out_shape=jax.ShapeDtypeStruct((high.shape[0], width), BF16),
        compiler_params=pltpu.CompilerParams(vmem_limit_bytes=VMEM_LIMIT),
        name="combine",
    )(high, low, rows)


def routing(routes, gate_ints, modality, capacity):
    tokens = routes.shape[0]
    key = (routes * 2 + modality[:, None]).reshape(-1)
    order = jnp.arange(2 * tokens, dtype=jnp.int32)
    same = (key[:, None] == key[None, :]) & (order[None, :] < order[:, None])
    rank = jnp.sum(same.astype(jnp.int32), 1)
    hot = key[:, None] == jnp.arange(2 * EXPERTS, dtype=jnp.int32)[None, :]
    limit = jnp.sum(jnp.where(hot, capacity.reshape(1, -1), 0), 1)
    spot = jnp.where(rank < limit, key * CAP + rank, -1).reshape(tokens, 2)
    slot = jnp.arange(EXPERTS * SLOTS, dtype=jnp.int32)
    select = (spot[None, :, 0] == slot[:, None]) | (spot[None, :, 1] == slot[:, None])
    place = spot[:, :, None] == slot[None, None, :]
    low = gate_ints % 8
    high = jnp.sum(jnp.where(place, (gate_ints - low)[:, :, None], 0), 1)
    low = jnp.sum(jnp.where(place, low[:, :, None], 0), 1)
    to_gate = lambda v: (v.astype(F32) / 1024.0).astype(BF16)
    return select.astype(BF16), to_gate(high), to_gate(low)


def body(
    residual,
    queries,
    keys,
    values,
    out_proj,
    norm_gain,
    expert_in,
    expert_down,
    routes,
    gate_ints,
    modality,
    capacity,
):
    devices = lax.axis_size("seq")
    pos = lax.axis_index("seq")
    rows, width = residual.shape
    back = (WINDOW + rows - 1) // rows
    blocks = window_blocks(jnp.concatenate([keys, values], 1), pos, back)
    offsets = jnp.stack([jnp.where(b < 0, 4 * back, pos - b) for _, b in blocks]).astype(jnp.int32)
    select, high, low = routing(routes, gate_ints, modality, capacity)
    gain = norm_gain.reshape(1, width)
    shard = out_proj.shape[1]
    if back == 8 and devices % back == 0 and shard % 16 == 0 and back * shard % HEAD == 0:
        found = gather_weight(out_proj.T, back)
        where = jnp.stack([pos // back, pos % back // 2, pos % 2]).astype(jnp.int32)
        context = attention(queries, [v for v, _ in blocks], offsets)
        mine, send = project_half(where, context, swap(context, 1), found)
        attended, slots = merge(where, mine, swap(send, 1), residual, gain, select, shard)
    else:
        weight_t = lax.all_gather(out_proj.T, "seq", axis=0, tiled=True)
        context = attention(queries, [v for v, _ in blocks], offsets)
        attended, slots = project(context, weight_t, residual, gain, select)
    ways = max(1, devices // EXPERTS)
    local = max(1, EXPERTS // devices)
    if ways > 1:
        slots = jnp.repeat(slots.reshape(EXPERTS, SLOTS, width), ways, 0)
    outgoing = slots.reshape(devices, local * SLOTS, width)
    arrived = lax.all_to_all(outgoing, "seq", split_axis=0, concat_axis=0, tiled=True)
    arrived = arrived.reshape(devices * local * SLOTS, width)
    if expert_in.shape[2] % (local * HEAD) == 0:
        computed = experts(arrived, expert_in, expert_down, local)
    else:
        computed = experts_plain(arrived, expert_in, expert_down, local)
    computed = lax.optimization_barrier(computed)
    returned = lax.all_to_all(
        computed.reshape(devices, local * SLOTS, width), "seq", split_axis=0, concat_axis=0, tiled=True
    )
    if ways > 1:
        parts = returned.reshape(EXPERTS, ways, SLOTS, width).astype(F32)
        returned = jnp.sum(parts, 1).astype(BF16)
    expert_mix = combine(high, low, returned.reshape(EXPERTS * SLOTS, width))
    return (attended, expert_mix)


def solution(mesh):
    placed = (
        P("seq", None),
        P("seq", None),
        P("seq", None),
        P("seq", None),
        P(None, "seq"),
        P(),
        P(None, None, "seq"),
        P("seq", None),
        P("seq", None),
        P("seq", None),
        P("seq"),
        P(),
    )
    return jax.shard_map(
        body,
        mesh=mesh,
        in_specs=placed,
        out_specs=(P("seq", None), P("seq", None)),
        check_vma=False,
    )
```
